32 devices in a mesh: row: 2 (over core), col: 4 (over y, x), depth: 4 (over z).
Axes of the slice: x: 2, y: 2, z: 4, core: 2. Of those that a mesh axis runs over, the one named last changes fastest.
Arguments:
- normed: bfloat16 [512, 4, 4608], P('col', 'depth', 'row'), may hold values from -6 to 6
- qkv_grad: bfloat16 [512, 4, 8192], P('row', 'depth', 'col'), may hold values from -0.1875 to 0.1875
- attn_out: bfloat16 [512, 4, 4096], P('col', 'depth', 'row'), may hold values from -6 to 6
- out_grad: bfloat16 [512, 4, 4608], P('row', 'depth', 'col'), may hold values from -0.1875 to 0.1875
Outputs:
- qkv_weight_grad: float32 [4608, 8192], P('row', ('col', 'depth'))
- o_weight_grad: float32 [4096, 4608], P('row', ('col', 'depth'))
The draws below stay inside these ranges and needn't reach their ends.
All inputs are finite; a program needn't handle non-finite values.
Results may differ from the reference program's by a relative error of at most 0.0003.
Values may be sent and summed in bfloat16 or wider, within the bound.
No kernel may reach another device: no remote copies, remote signals or barrier semaphores. Data moves between devices by JAX's collectives and lax.ppermute only.
A program may use at most 128 MiB of HBM per device.

```python
import jax
import jax.numpy as jnp
from jax import lax

D = 4608
QKV = 8192
HQW = 4096
TOK_DEPTH = 512
TOKENS = 2048
N_DEPTH = 4


def spiked(array, own_key, source, target, parts, factor):
    owner, partner = [(jnp.arange(array.shape[dim]) // (array.shape[dim] // parts)).reshape([-1 if axis == dim else 1 for axis in range(array.ndim)]) for dim in (source, target)]
    chosen = jax.random.permutation(own_key, parts)[partner]
    strong = (owner == chosen) | (owner == (partner + parts // 2) % parts)
    return jnp.where(strong, factor * array, array)


def block_levels(key, dims, pieces, smallest, top_value):
    loudness = 1.0
    for dim, blocks in pieces:
        draws = jax.random.uniform(jax.random.fold_in(jax.random.fold_in(key, 6), dim), (blocks,), jnp.float32, smallest / len(pieces), top_value / len(pieces))
        loudness = loudness * jnp.repeat(jnp.exp(draws), dims[dim] // blocks).reshape((-1,) + (1,) * (len(dims) - 1 - dim))
    return loudness


def centred(rng, shape, spread, reach, shards=(), kind=jnp.bfloat16):
    drawn = jax.random.normal(rng, shape, jnp.float32) * spread
    if len(shards) > 0:
        drawn = block_levels(rng, shape, shards, -0.22, 0.18) * drawn
    return jnp.clip(drawn, min=-reach, max=reach).astype(kind)


def noise_with(own_key, dims, scale, bound, split, heavy, kind=jnp.bfloat16):
    entries = scale * jax.random.normal(own_key, dims, jnp.float32)
    if split:
        entries = entries * block_levels(own_key, dims, split, -0.22, 0.18)
    return jnp.clip(spiked(entries, jax.random.fold_in(own_key, 3), *heavy), -bound, bound).astype(kind)


def setup_inputs(seed: int = 0) -> dict:
    key_list = jax.random.split(jax.random.key(seed), 5)
    normed = centred(key_list[0], (TOK_DEPTH, N_DEPTH, D), 1.0, 6.0, ((0, 4), (1, 4), (2, 2)))
    qkv_grad = noise_with(key_list[1], (TOK_DEPTH, N_DEPTH, QKV), (TOKENS ** -0.5), 0.1875, ((0, 2), (1, 4), (2, 4)), (1, 2, 4, 2.0))
    attn_out = centred(key_list[2], (TOK_DEPTH, N_DEPTH, HQW), 1.0, 6.0, ((0, 4), (1, 4), (2, 2)))
    out_grad = noise_with(key_list[3], (TOK_DEPTH, N_DEPTH, D), (TOKENS ** -0.5), 0.1875, ((0, 2), (1, 4), (2, 4)), (1, 2, 4, 2.0))
    return {"normed": normed, "qkv_grad": qkv_grad, "attn_out": attn_out, "out_grad": out_grad}


def outer_sum(left, right):
    return lax.dot_general(left, right, (((0, 1), (0, 1)), ((), ())), preferred_element_type=jnp.float32)


def reference(normed, qkv_grad, attn_out, out_grad):
    qkv_weight_grad = outer_sum(normed, qkv_grad)
    o_weight_grad = outer_sum(attn_out, out_grad)
    return (qkv_weight_grad, o_weight_grad)
```

```python
import jax
import jax.numpy as jnp
from jax import lax
from jax.sharding import PartitionSpec as P


def outer_sum(left, right):
    return lax.dot_general(
        left, right, (((0,), (0,)), ((), ())), preferred_element_type=jnp.float32
    )


def flatten(block):
    return block.reshape(block.shape[0] * block.shape[1], block.shape[2])


def reduced_total(left, right):
    lefts = lax.all_gather(flatten(left), "col", axis=0, tiled=True)
    partial = outer_sum(lefts, lax.all_gather(flatten(right), "row", axis=0, tiled=True))
    return lax.psum_scatter(partial, "depth", scatter_dimension=1, tiled=True)


def reduce_plan(normed, qkv_grad, attn_out, out_grad):
    return reduced_total(normed, qkv_grad), reduced_total(attn_out, out_grad)


def flip(block, bits, cols):
    return lax.ppermute(block, "col", [(c, c ^ bits) for c in range(cols)])


def shift(block, step, depths):
    return lax.ppermute(block, "depth", [(z, (z + step) % depths) for z in range(depths)])


def gather_plan(mesh_shape, normed, qkv_grad, attn_out, out_grad):
    rows, cols, depths = (mesh_shape[a] for a in ("row", "col", "depth"))
    me_z = lax.axis_index("depth")
    me_c = lax.axis_index("col")
    me_r = lax.axis_index("row")
    left_n, left_a = flatten(normed), flatten(attn_out)
    right_n, right_a = flatten(qkv_grad), flatten(out_grad)
    wide_n, wide_a = right_n.shape[1] // depths, right_a.shape[1] // depths
    tokens = left_n.shape[0]

    def columns(block, wide, step):
        target = lax.rem(me_z + step, depths)
        return lax.dynamic_slice_in_dim(block, target * wide, wide, axis=1)

    steps = [0] + sorted(range(1, depths), key=lambda s: min(s, depths - s))
    pieces_n = {s: shift(left_n, s, depths) if s else left_n for s in steps}
    pieces_a = {s: shift(left_a, s, depths) if s else left_a for s in steps}
    grads = {}
    for s in steps:
        both = jnp.concatenate(
            [columns(right_n, wide_n, s), columns(right_a, wide_a, s)], axis=1
        )
        grads[s] = shift(both, s, depths) if s else both
    mine = jnp.stack([grads[s] for s in steps])
    other = lax.ppermute(mine, "row", [(0, 1), (1, 0)])
    low = jnp.where(me_r == 0, mine, other)
    high = jnp.where(me_r == 0, other, mine)
    whole = jnp.concatenate([low, high], axis=1)

    total_n = total_a = None
    for k, s in enumerate(steps):
        n0, a0 = pieces_n[s], pieces_a[s]
        n1, a1 = flip(n0, 1, cols), flip(a0, 1, cols)
        n2, a2 = flip(n0, 2, cols), flip(a0, 2, cols)
        n3, a3 = flip(n1, 2, cols), flip(a2, 1, cols)
        right = jnp.concatenate(
            [
                lax.dynamic_slice_in_dim(whole[k], (me_c ^ b) * tokens, tokens, axis=0)
                for b in range(cols)
            ]
        )
        part_n = outer_sum(jnp.concatenate([n0, n1, n2, n3]), right[:, :wide_n])
        part_a = outer_sum(jnp.concatenate([a0, a1, a2, a3]), right[:, wide_n:])
        total_n = part_n if total_n is None else total_n + part_n
        total_a = part_a if total_a is None else total_a + part_a
    return total_n, total_a


def solution(mesh):
    shape = dict(mesh.shape)

    def per_device(normed, qkv_grad, attn_out, out_grad):
        gathered = 2 * shape["col"] * shape["depth"] * (normed.size + attn_out.size)
        reduced = 4 * (
            normed.shape[2] * qkv_grad.shape[2] + attn_out.shape[2] * out_grad.shape[2]
        )
        if shape["row"] == 2 and shape["col"] == 4 and gathered < reduced:
            return gather_plan(shape, normed, qkv_grad, attn_out, out_grad)
        return reduce_plan(normed, qkv_grad, attn_out, out_grad)

    in_specs = (
        P("col", "depth", "row"),
        P("row", "depth", "col"),
        P("col", "depth", "row"),
        P("row", "depth", "col"),
    )
    out_specs = (P("row", ("col", "depth")), P("row", ("col", "depth")))
    return jax.shard_map(
        per_device, mesh=mesh, in_specs=in_specs, out_specs=out_specs, check_vma=False
    )
```

```python
import jax
import jax.numpy as jnp
from jax import lax
from jax.sharding import PartitionSpec as P


def outer_sum(left, right):
    return lax.dot_general(
        left, right, (((0,), (0,)), ((), ())), preferred_element_type=jnp.float32
    )


def flatten(block):
    return block.reshape(block.shape[0] * block.shape[1], block.shape[2])


def reduced_total(left, right):
    lefts = lax.all_gather(flatten(left), "col", axis=0, tiled=True)
    partial = outer_sum(lefts, lax.all_gather(flatten(right), "row", axis=0, tiled=True))
    return lax.psum_scatter(partial, "depth", scatter_dimension=1, tiled=True)


def reduce_plan(normed, qkv_grad, attn_out, out_grad):
    return reduced_total(normed, qkv_grad), reduced_total(attn_out, out_grad)


def flip(block, bits):
    return lax.ppermute(block, "col", [(c, c ^ bits) for c in range(4)])


def shift(block, step):
    return lax.ppermute(block, "depth", [(z, (z + step) % 4) for z in range(4)])


def along_depth(block, me_z):
    ahead = shift(block, 1)
    behind = shift(block, 3)
    up = lax.ppermute(ahead, "depth", [(1, 2), (2, 3)])
    down = lax.ppermute(behind, "depth", [(1, 0), (2, 1)])
    across = jnp.where(me_z >= 2, up, down)
    return [block, ahead, across, behind]


def in_plane(block, far_by_y):
    by_x = flip(block, 1)
    by_y = flip(block, 2)
    far = flip(by_x, 2) if far_by_y else flip(by_y, 1)
    return [block, by_x, by_y, far]


def gather_plan(normed, qkv_grad, attn_out, out_grad):
    me_z = lax.axis_index("depth")
    me_c = lax.axis_index("col")
    me_r = lax.axis_index("row")
    side = me_c & 1
    left_n, left_a = flatten(normed), flatten(attn_out)
    right_n, right_a = flatten(qkv_grad), flatten(out_grad)
    tokens, half = left_a.shape[0], left_a.shape[1] // 2

    def columns(block, step):
        wide = block.shape[1] // 4
        target = lax.rem(me_z + step, 4)
        return lax.dynamic_slice_in_dim(block, target * wide, wide, axis=1)

    def over_depth(block):
        turned = [shift(columns(block, s), s) for s in (1, 2, 3)]
        own = columns(block, 0)
        return jnp.stack([own] + turned)

    def rows(block):
        other = lax.ppermute(block, "row", [(0, 1), (1, 0)])
        both = jnp.concatenate([block, other], axis=1)
        seat = (me_c & 2) ^ (2 * me_r)
        starts = [tokens * ((seat ^ (b & 2)) + (side ^ (b & 1))) for b in range(4)]
        return jnp.concatenate(
            [lax.dynamic_slice_in_dim(both, at, tokens, axis=1) for at in starts],
            axis=1,
        )

    def total(pieces, rights, early, late):
        def part(s):
            return outer_sum(jnp.concatenate(pieces[s]), rights[s])

        first = sum(part(s) for s in early[1:]) + part(early[0])
        first = lax.optimization_barrier(first)
        return first + sum(part(s) for s in late)

    def features(which):
        return lax.dynamic_slice_in_dim(left_a, which * half, half, axis=1)

    blocks_n = along_depth(left_n, me_z)
    all_n = [in_plane(blocks_n[s], s in (3, 2)) for s in range(4)]

    kept, sent = features(side), features(1 - side)
    partner = flip(sent, 1)
    pair = jnp.concatenate([kept, partner])
    blocks_a = along_depth(pair, me_z)
    all_a = [[blocks_a[s], flip(blocks_a[s], 2)] for s in range(4)]

    grad_a = over_depth(right_a)
    far_a = rows(flip(grad_a, 1))
    grad_a = rows(grad_a)
    theirs = total(all_a, [far_a[s] for s in range(4)], (0, 1, 3), (2,))
    ours = total(all_a, [grad_a[s] for s in range(4)], (0, 1, 3), (2,))
    theirs = flip(theirs, 1)
    first = jnp.where(side == 0, ours, theirs)
    second = jnp.where(side == 0, theirs, ours)
    total_a = jnp.concatenate([first, second])

    grad_n = rows(over_depth(right_n))
    total_n = total(all_n, [grad_n[s] for s in range(4)], (0, 1, 3), (2,))
    return total_n, total_a


def solution(mesh):
    shape = dict(mesh.shape)

    def per_device(normed, qkv_grad, attn_out, out_grad):
        if shape == {"row": 2, "col": 4, "depth": 4}:
            return gather_plan(normed, qkv_grad, attn_out, out_grad)
        return reduce_plan(normed, qkv_grad, attn_out, out_grad)

    in_specs = (
        P("col", "depth", "row"),
        P("row", "depth", "col"),
        P("col", "depth", "row"),
        P("row", "depth", "col"),
    )
    out_specs = (P("row", ("col", "depth")), P("row", ("col", "depth")))
    return jax.shard_map(
        per_device, mesh=mesh, in_specs=in_specs, out_specs=out_specs, check_vma=False
    )
```
